32 devices in a mesh: grp: 4 (over z), dev: 8 (over y, x, core).
Axes of the slice: x: 2, y: 2, z: 4, core: 2. Of those that a mesh axis runs over, the one named last changes fastest.
Arguments:
- a_blocks: bfloat16 [1024, 7, 192, 192], P(('grp', 'dev')), may hold values from -0.4375 to 0.4375
- prolong_t: bfloat16 [1024, 32, 192], P(('grp', 'dev')), may hold values from -1.796875 to 1.796875
- elem_slot: int32 [1024], P(('grp', 'dev')), may hold values from 0 to 5, as said below
- touch_agg: int32 [32, 6], replicated, may hold values from 0 to 135, as said below
- nbr: int32 [1024, 6], P(('grp', 'dev')), may hold values from -1 to 1023, as said below
- nbr_agg: int32 [1024, 6], P(('grp', 'dev')), may hold values from -1 to 135, as said below
- coarse_row: int32 [136], replicated, may hold values from 0 to 191, as said below
Outputs:
- coarse: float32 [192, 7, 1024], P('dev')
The draws below stay inside these ranges and needn't reach their ends.
Inputs may be any that keep to these rules, and one draw needn't show every extreme that they name: Element e lies on device e // 32 (devices numbered grp-major). elem_slot[e] is the position of e's aggregate in touch_agg[e // 32]. `touch_agg`: each row lists 6 distinct aggregates, exactly those of the device's elements; all devices that touch one aggregate share their grp index. `nbr`: global element index across each face, or -1 on the domain's boundary; adjacency is symmetric; a neighbour lies on the same device, or on the device whose grp index differs by one (same dev index), or whose dev index differs by one (same grp index); exactly 8 elements of a device have a neighbour on each existing device next along grp, and exactly 8 on each existing device next along dev. `nbr_agg`: the aggregate of the element nbr[e, f], -1 exactly where nbr[e, f] is -1. Distinct values; aggregate a's row belongs to dev index coarse_row[a] // 24. Of the aggregates touched by one device at most 1 belong to one dev index, and of those touched by the devices of one grp index at most 6; one dev index reaches both bounds and holds 24 rows.
All inputs are finite; a program needn't handle non-finite values.
Results may differ from the reference program's by a relative error of at most 0.005.
Values may be sent and summed in bfloat16 or wider, within the bound.
A program may use at most 128 MiB of HBM per device.

```python
import jax
import jax.numpy as jnp
from jax import lax

B = 192
C = 32
EX = 4
EY = 4
EZ = 2
E_DEV = 32
ELEMS = 1024
TOUCH = 6
SEND_CAP = 1
NYBOX = 17
AGG = 136
ROWS_OWN = 24
COARSE = 192
N_GRP = 4
N_DEV = 8


def face_fields(field):
    padded = jnp.pad(field, 1, constant_values=-1)
    return jnp.stack([padded[:-2, 1:-1, 1:-1], padded[2:, 1:-1, 1:-1], padded[1:-1, :-2, 1:-1], padded[1:-1, 2:, 1:-1], padded[1:-1, 1:-1, :-2], padded[1:-1, 1:-1, 2:]], axis=-1)


def geometry(key):
    keys = jax.random.split(jax.random.fold_in(key, 11), 6)
    devices = N_GRP * N_DEV
    half_x = EX // 2
    half_y = EY // 2
    span_y = half_y + 1
    half_z = EZ // 2
    coord_x, coord_y, coord_z = jnp.meshgrid(jnp.arange(N_GRP * EX, dtype=jnp.int32), jnp.arange(N_DEV * EY, dtype=jnp.int32), jnp.arange(EZ, dtype=jnp.int32), indexing='ij')
    grp_of = coord_x // EX
    dev_of = coord_y // EY
    device = grp_of * N_DEV + dev_of
    canon = (coord_x % EX * EY + coord_y % EY) * EZ + coord_z
    local_perms = jax.vmap(lambda k: jax.random.permutation(k, E_DEV))(jax.random.split(keys[0], devices))
    global_id = (device * E_DEV + local_perms[device, canon]).astype(jnp.int32)
    box_x = coord_x // 2
    box_y = (coord_y + 1) // 2
    box_z = coord_z // 2
    box = (box_x * NYBOX + box_y) * half_z + box_z
    box_perm = jax.random.permutation(keys[1], AGG).astype(jnp.int32)
    agg = box_perm[box]
    canon_touch = ((box_x - grp_of * half_x) * span_y + (box_y - dev_of * half_y)) * half_z + box_z
    touch_perms = jax.vmap(lambda k: jax.random.permutation(k, TOUCH))(jax.random.split(keys[2], devices))
    slot = touch_perms[device, canon_touch].astype(jnp.int32)
    touch = jnp.zeros((devices, TOUCH), jnp.int32).at[device, slot].set(agg)
    classes = jnp.arange(TOUCH, dtype=jnp.int32)
    class_ry = classes // half_z % span_y
    shuffled = jax.random.permutation(keys[3], TOUCH).astype(jnp.int32)
    score = jnp.where(class_ry != 0, TOUCH, 0) + shuffled
    order = jnp.argsort(score, stable=True)
    class_rank = jnp.zeros((TOUCH,), jnp.int32).at[order].set(classes)
    owner_perm = jax.random.permutation(keys[4], N_DEV).astype(jnp.int32)
    owner_class = jnp.where(class_rank < SEND_CAP, owner_perm[0], owner_perm[1 + (class_rank - SEND_CAP) % (N_DEV - 1)])
    grid_x, grid_y, grid_z = jnp.meshgrid(jnp.arange(N_GRP * half_x, dtype=jnp.int32), jnp.arange(NYBOX, dtype=jnp.int32), jnp.arange(half_z, dtype=jnp.int32), indexing='ij')
    class_box = ((grid_x % half_x * span_y + grid_y % span_y) * half_z + grid_z).reshape(-1)
    owner_box = owner_class[class_box]
    priority = jax.random.permutation(keys[5], AGG).astype(jnp.int32)
    earlier = (owner_box[None, :] == owner_box[:, None]) & (priority[None, :] < priority[:, None])
    position = jnp.sum(earlier.astype(jnp.int32), axis=1)
    row_box = (owner_box * ROWS_OWN + position).astype(jnp.int32)
    coarse_rows = jnp.zeros((AGG,), jnp.int32).at[box_perm].set(row_box)
    flat_ids = global_id.reshape(-1)
    elem_slots = jnp.zeros((ELEMS,), jnp.int32).at[flat_ids].set(slot.reshape(-1))
    neighbours = jnp.zeros((ELEMS, 6), jnp.int32).at[flat_ids].set(face_fields(global_id).reshape(-1, 6))
    neighbour_aggs = jnp.zeros((ELEMS, 6), jnp.int32).at[flat_ids].set(face_fields(agg).reshape(-1, 6))
    return (elem_slots, touch, neighbours, neighbour_aggs, coarse_rows)


def draw_elem_slot(key, part):
    return geometry(key)[0]


def draw_touch_agg(key, part):
    return geometry(key)[1]


def draw_nbr(key, part):
    return geometry(key)[2]


def draw_nbr_agg(key, part):
    return geometry(key)[3]


def draw_coarse_row(key, part):
    return geometry(key)[4]


def level_of(rng, shape, cuts, smallest, top_value):
    gain, own = 1.0, jax.random.fold_in(rng, 6)
    for axis_at, blocks in cuts:
        steps = jnp.exp(jax.random.uniform(jax.random.fold_in(own, axis_at), (blocks,), jnp.float32, smallest / len(cuts), top_value / len(cuts)))
        gain = gain * jnp.repeat(steps, shape[axis_at] // blocks).reshape([-1 if axis == axis_at else 1 for axis in range(len(shape))])
    return gain


def centred(stream_key, dims, scale, bound, shards=(), kind=jnp.bfloat16):
    result = jax.random.normal(stream_key, dims, jnp.float32) * scale
    if len(shards) > 0:
        result = level_of(stream_key, dims, shards, -0.22, 0.18) * result
    return jnp.clip(result, min=-bound, max=bound).astype(kind)


def setup_inputs(seed: int = 0) -> dict:
    streams_of = jax.random.split(jax.random.key(seed), 8)
    a_blocks = centred(streams_of[0], (ELEMS, 7, B, B), B ** -0.5, 0.4375, ((0, 32),))
    prolong_t = centred(streams_of[1], (ELEMS, C, B), 0.3, 1.796875, ((0, 32),))
    elem_slot = draw_elem_slot(jax.random.fold_in(streams_of[7], 71), 0)
    touch_agg = draw_touch_agg(jax.random.fold_in(streams_of[7], 71), 0)
    nbr = draw_nbr(jax.random.fold_in(streams_of[7], 71), 0)
    nbr_agg = draw_nbr_agg(jax.random.fold_in(streams_of[7], 71), 0)
    coarse_row = draw_coarse_row(jax.random.fold_in(streams_of[7], 71), 0)
    return dict(a_blocks=a_blocks, prolong_t=prolong_t, elem_slot=elem_slot, touch_agg=touch_agg, nbr=nbr, nbr_agg=nbr_agg, coarse_row=coarse_row)


def reference(a_blocks, prolong_t, elem_slot, touch_agg, nbr, nbr_agg, coarse_row):
    elems = a_blocks.shape[0]
    devices = elems // E_DEV
    owner_device = (jnp.arange(elems, dtype=jnp.int32) // E_DEV).astype(jnp.int32)
    agg_of = touch_agg[owner_device, elem_slot]
    valid = nbr >= 0
    safe_nbr = jnp.where(valid, nbr, 0).astype(jnp.int32)

    def per_device(index):
        start = (index * E_DEV).astype(jnp.int32)
        blocks = lax.dynamic_slice_in_dim(a_blocks, start, E_DEV, 0).astype(jnp.float32)
        left = lax.dynamic_slice_in_dim(prolong_t, start, E_DEV, 0)
        left_blocks = jnp.einsum("ecb,ekbd->ekcd", left.astype(jnp.float32), blocks,
                                 precision=lax.Precision.HIGHEST).astype(jnp.bfloat16)
        across = lax.dynamic_slice_in_dim(safe_nbr, start, E_DEV, 0)
        right = jnp.concatenate([left[:, None], prolong_t[across]], axis=1)
        products = jnp.einsum("ekcd,ekxd->ekcx", left_blocks.astype(jnp.float32), right.astype(jnp.float32),
                              precision=lax.Precision.HIGHEST)
        return products.reshape(E_DEV, 7, C * C)

    products = lax.map(per_device, jnp.arange(devices, dtype=jnp.int32)).reshape(elems, 7, C * C)
    same = valid & (nbr_agg == agg_of[:, None])
    apart = valid & jnp.logical_not(same)
    faces = products[:, 1:]
    diagonal = products[:, 0] + jnp.sum(jnp.where(same[:, :, None], faces, jnp.float32(0.0)), axis=1)
    contrib = jnp.concatenate([diagonal[:, None], jnp.where(apart[:, :, None], faces, jnp.float32(0.0))], axis=1)
    coarse_sum = jax.ops.segment_sum(contrib, agg_of, num_segments=AGG)
    coarse = jnp.zeros((COARSE, 7, C * C), jnp.float32).at[coarse_row].set(coarse_sum)
    return coarse
```

```python
import functools

import jax
import jax.numpy as jnp
from jax import lax
from jax.experimental import pallas as pl
from jax.experimental.pallas import tpu as pltpu
from jax.sharding import PartitionSpec as P

EX = 4
EY = 4
MESH = pl.DeviceIdType.MESH
F32 = jnp.float32
BF16 = jnp.bfloat16


def iota(shape, dim):
    return lax.broadcasted_iota(jnp.int32, shape, dim)


def kernel(
    n_grp, n_dev, halo, group_rows,
    sidx, wf, slot, tinv, pos, cidx,
    a_ref, p_ref, ms_ref, ma_ref,
    out_ref,
    a_buf, pool, pack, left, prod_s, prod_a, part_t, parts, inbox, gathered, flat,
    a_sem, h_send, h_recv, x_send, x_recv, g_send, g_recv,
):
    grp = lax.axis_index("grp")
    dev = lax.axis_index("dev")
    e_dev, width_c, width_b = p_ref.shape
    n_k = a_ref.shape[1]
    touch = part_t.shape[0] - 1
    rows_own = out_ref.shape[0]
    wide = n_k * width_c
    lane = 128
    rep = lane // width_c
    sub = width_c // rep

    def a_copy(e):
        return pltpu.make_async_copy(a_ref.at[e], a_buf.at[e], a_sem.at[e])

    @pl.loop(0, e_dev)
    def _(e):
        a_copy(e).start()

    barrier = pltpu.get_barrier_semaphore()
    for off in range(1, n_dev):
        pl.semaphore_signal(
            barrier, inc=1, device_id=(grp, lax.rem(dev + off, n_dev)), device_id_type=MESH
        )
    for off in range(1, n_grp):
        pl.semaphore_signal(
            barrier, inc=1, device_id=(lax.rem(grp + off, n_grp), dev), device_id_type=MESH
        )

    for j in range(4 * halo):
        pack[j] = p_ref[sidx[j]]
    pool[0:e_dev] = p_ref[...]
    pl.semaphore_wait(barrier, n_dev + n_grp - 2)

    dirs = (
        (grp > 0, (grp - 1, dev)),
        (grp < n_grp - 1, (grp + 1, dev)),
        (dev > 0, (grp, dev - 1)),
        (dev < n_dev - 1, (grp, dev + 1)),
    )

    def halo_copy(d, target):
        back = d ^ 1
        return pltpu.make_async_remote_copy(
            src_ref=pack.at[pl.ds(d * halo, halo)],
            dst_ref=pool.at[pl.ds(e_dev + back * halo, halo)],
            send_sem=h_send.at[d],
            recv_sem=h_recv.at[back],
            device_id=target,
            device_id_type=MESH,
        )

    for d, (there, target) in enumerate(dirs):
        @pl.when(there)
        def _(d=d, target=target):
            halo_copy(d, target).start()

    @pl.loop(0, e_dev)
    def _(e):
        a_copy(e).wait()
        own = p_ref[e]
        for k in range(n_k):
            left[e, k * width_c:(k + 1) * width_c, :] = jnp.dot(
                own, a_buf[e, k], preferred_element_type=F32
            ).astype(BF16)

    for d, (there, target) in enumerate(dirs):
        @pl.when(there)
        def _(d=d, target=target):
            halo_copy(d, target).wait_send()
            pltpu.make_async_remote_copy(
                src_ref=pack.at[pl.ds(d * halo, halo)],
                dst_ref=pool.at[pl.ds(e_dev + d * halo, halo)],
                send_sem=h_send.at[d],
                recv_sem=h_recv.at[d],
                device_id=target,
                device_id_type=MESH,
            ).wait_recv()

    group_of_lane = iota((width_c, wide), 1) // width_c

    @pl.loop(0, e_dev)
    def _(e):
        right = jnp.concatenate(
            [pool[e]] + [pool[wf[e * (n_k - 1) + f]] for f in range(n_k - 1)], axis=0
        )
        full = lax.dot_general(
            left[e], right, (((1,), (1,)), ((), ())), preferred_element_type=F32
        )
        picked = full[0:width_c]
        for k in range(1, n_k):
            picked = jnp.where(group_of_lane == k, full[k * width_c:(k + 1) * width_c], picked)
        prod_s[e] = jnp.where(ms_ref[pl.ds(e, 1), :] > 0, picked, 0.0)
        prod_a[e] = jnp.where(ma_ref[pl.ds(e, 1), :] > 0, picked, 0.0)

    spread_s = (iota((wide, lane), 0) % width_c == iota((wide, lane), 1) % width_c).astype(F32).astype(BF16)
    rest = (n_k - 1) * lane
    spread_a = (
        iota((wide, rest), 0)
        == (iota((wide, rest), 1) // lane + 1) * width_c + iota((wide, rest), 1) % width_c
    ).astype(F32).astype(BF16)
    keep = iota((width_c, n_k * lane), 0) % rep == (iota((width_c, n_k * lane), 1) % lane) // width_c
    squeeze = (iota((sub, width_c), 1) // rep == iota((sub, width_c), 0)).astype(F32).astype(BF16)

    part_t[touch] = jnp.zeros(part_t.shape[1:], BF16)

    def spread(value, table):
        high = value.astype(BF16)
        low = (value - high.astype(F32)).astype(BF16)
        return jnp.dot(high, table, preferred_element_type=F32) + jnp.dot(
            low, table, preferred_element_type=F32
        )

    for t in range(touch):
        zero = jnp.zeros((width_c, wide), F32)

        def add(e, sums, t=t):
            sum_s, sum_a = sums
            member = jnp.where(slot[e] == t, 1.0, 0.0).astype(F32)
            return sum_s + prod_s[e] * member, sum_a + prod_a[e] * member

        sum_s, sum_a = lax.fori_loop(0, e_dev, add, (zero, zero), unroll=4)
        both = jnp.concatenate([spread(sum_s, spread_s), spread(sum_a, spread_a)], axis=1)
        both = jnp.where(keep, both, 0.0).astype(BF16)
        rows = jnp.dot(squeeze, both, preferred_element_type=F32)
        rows = jnp.concatenate([rows[:, s * lane:(s + 1) * lane] for s in range(n_k)], axis=0)
        part_t[t] = rows.astype(BF16)

    for o in range(n_dev):
        parts[o] = part_t[tinv[o]]
    inbox[dev] = parts[dev]

    def part_copy(off):
        target = lax.rem(dev + off, n_dev)
        return pltpu.make_async_remote_copy(
            src_ref=parts.at[target],
            dst_ref=inbox.at[dev],
            send_sem=x_send.at[off],
            recv_sem=x_recv.at[off],
            device_id=(grp, target),
            device_id_type=MESH,
        )

    def part_arrival(off):
        sender = lax.rem(dev + n_dev - off, n_dev)
        return pltpu.make_async_remote_copy(
            src_ref=parts.at[sender],
            dst_ref=inbox.at[sender],
            send_sem=x_send.at[off],
            recv_sem=x_recv.at[off],
            device_id=(grp, sender),
            device_id_type=MESH,
        )

    for off in range(1, n_dev):
        part_copy(off).start()
    for off in range(1, n_dev):
        part_arrival(off).wait_recv()

    for j in range(group_rows):
        total = jnp.zeros(parts.shape[1:], F32)
        for d in range(n_dev):
            member = jnp.where(pos[d] == j, 1.0, 0.0).astype(F32)
            total = total + inbox[d].astype(F32) * member
        gathered[grp, j] = total.astype(BF16)

    def row_copy(off):
        target = lax.rem(grp + off, n_grp)
        return pltpu.make_async_remote_copy(
            src_ref=gathered.at[grp],
            dst_ref=gathered.at[grp],
            send_sem=g_send.at[off],
            recv_sem=g_recv.at[off],
            device_id=(target, dev),
            device_id_type=MESH,
        )

    def row_arrival(off):
        sender = lax.rem(grp + n_grp - off, n_grp)
        return pltpu.make_async_remote_copy(
            src_ref=gathered.at[sender],
            dst_ref=gathered.at[sender],
            send_sem=g_send.at[off],
            recv_sem=g_recv.at[off],
            device_id=(sender, dev),
            device_id_type=MESH,
        )

    for off in range(1, n_grp):
        row_copy(off).start()
    for off in range(1, n_grp):
        row_arrival(off).wait_recv()

    @pl.loop(0, rows_own)
    def _(r):
        at = cidx[r]
        safe = jnp.maximum(at, 0)
        row = gathered[safe // group_rows, safe % group_rows].astype(F32)
        flat[r] = jnp.where(at >= 0, row, 0.0)
        for j in range(sub):
            out_ref[r, :, j * lane:(j + 1) * lane] = flat[r, pl.ds(j, n_k, stride=sub), :]

    for off in range(1, n_dev):
        part_copy(off).wait_send()
    for off in range(1, n_grp):
        row_copy(off).wait_send()


def on_device(n_grp, n_dev, a_blocks, prolong_t, elem_slot, touch_agg, nbr, nbr_agg, coarse_row):
    grp = lax.axis_index("grp")
    dev = lax.axis_index("dev")
    device = grp * n_dev + dev
    e_dev, width_c, width_b = prolong_t.shape
    n_k = a_blocks.shape[1]
    touch = touch_agg.shape[1]
    halo = e_dev // EX
    half_y = EY // 2
    span_y = half_y + 1
    group_rows = (n_dev * half_y + 1 + half_y) // span_y
    rows_own = n_grp * group_rows
    assert touch <= n_dev
    i32 = jnp.int32

    def ar(n):
        return jnp.arange(n, dtype=i32)

    none = jnp.int32(-2)
    near = jnp.stack([
        jnp.where(grp > 0, device - n_dev, none),
        jnp.where(grp < n_grp - 1, device + n_dev, none),
        jnp.where(dev > 0, device - 1, none),
        jnp.where(dev < n_dev - 1, device + 1, none),
    ])
    source = jnp.where(nbr >= 0, nbr // e_dev, -1)
    local = nbr - source * e_dev
    hit = jnp.any(source[None] == near[:, None, None], axis=2).astype(i32)
    rank = jnp.sum(hit[:, None, :] * (ar(e_dev)[None, :] < ar(e_dev)[:, None]), axis=2)
    sidx = jnp.sum(
        jnp.where((rank[:, None, :] == ar(halo)[:, None]) & (hit[:, None, :] > 0), ar(e_dev), 0), axis=2
    ).reshape(-1)
    seen = jnp.any(
        nbr[None, None] == (near[:, None] * e_dev + ar(e_dev))[:, :, None, None], axis=(2, 3)
    ).astype(i32)
    behind = jnp.sum(
        jnp.where(
            source[:, :, None, None] == near[:, None],
            seen * (ar(e_dev) < local[:, :, None, None])
            + jnp.where(ar(e_dev) == 0, (e_dev + ar(4) * halo)[:, None], 0),
            0,
        ),
        axis=(2, 3),
    )
    wf = jnp.where(source == device, local, behind).reshape(-1)

    touched = lax.dynamic_index_in_dim(touch_agg, device, 0, keepdims=False)
    own_agg = jnp.sum(jnp.where(elem_slot[:, None] == ar(touch), touched, 0), axis=1)
    valid = nbr >= 0
    same = valid & (nbr_agg == own_agg[:, None])
    apart = valid & jnp.logical_not(same)
    true = jnp.ones((e_dev, 1), bool)
    ms = jnp.repeat(jnp.concatenate([true, same], axis=1).astype(F32), width_c, axis=1)
    ma = jnp.repeat(jnp.concatenate([~true, apart], axis=1).astype(F32), width_c, axis=1)

    targets = jnp.sum(
        jnp.where(touch_agg[:, :, None] == ar(coarse_row.shape[0]), coarse_row, 0), axis=2
    )
    owners = targets // rows_own
    mine = owners == dev
    place = jnp.where(mine, targets - owners * rows_own, -1)
    present = jnp.any(
        place.reshape(n_grp, n_dev * touch)[:, :, None] == ar(rows_own), axis=1
    ).astype(i32)
    cidx = jnp.sum(
        present[:, :, None]
        * (
            present[:, None, :] * (ar(rows_own)[None, :] < ar(rows_own)[:, None])
            + jnp.where(ar(rows_own) == 0, ar(n_grp)[:, None] * group_rows + 1, 0)[:, None, :]
        ),
        axis=(0, 2),
    ) - 1
    own_present = lax.dynamic_index_in_dim(present, grp, 0, keepdims=False)
    group_place = lax.dynamic_slice_in_dim(place, grp * n_dev, n_dev, 0)
    pos = jnp.sum(
        jnp.where(
            group_place[:, :, None] >= 0,
            own_present * (ar(rows_own) < group_place[:, :, None]) + (ar(rows_own) == 0),
            0,
        ),
        axis=(1, 2),
    ) - 1
    own_owner = lax.dynamic_index_in_dim(owners, device, 0, keepdims=False)
    tinv = touch + jnp.sum(
        jnp.where(own_owner[None, :] == ar(n_dev)[:, None], ar(touch) - touch, 0), axis=1
    )

    lane = 128
    flat_rows = n_k * width_c * width_c // lane
    smem = pl.BlockSpec(memory_space=pltpu.SMEM)
    vmem = pl.BlockSpec(memory_space=pltpu.VMEM)
    wide = n_k * width_c
    return pl.pallas_call(
        functools.partial(kernel, n_grp, n_dev, halo, group_rows),
        out_shape=jax.ShapeDtypeStruct((rows_own, n_k, width_c * width_c), F32),
        in_specs=[smem] * 6 + [pl.BlockSpec(memory_space=pl.ANY)] + [vmem] * 3,
        out_specs=vmem,
        scratch_shapes=[
            pltpu.VMEM(a_blocks.shape, BF16),
            pltpu.VMEM((e_dev + 4 * halo, width_c, width_b), BF16),
            pltpu.VMEM((4 * halo, width_c, width_b), BF16),
            pltpu.VMEM((e_dev, wide, width_b), BF16),
            pltpu.VMEM((e_dev, width_c, wide), F32),
            pltpu.VMEM((e_dev, width_c, wide), F32),
            pltpu.VMEM((touch + 1, flat_rows, lane), BF16),
            pltpu.VMEM((n_dev, flat_rows, lane), BF16),
            pltpu.VMEM((n_dev, flat_rows, lane), BF16),
            pltpu.VMEM((n_grp, group_rows, flat_rows, lane), BF16),
            pltpu.VMEM((rows_own, flat_rows, lane), F32),
            pltpu.SemaphoreType.DMA((e_dev,)),
            pltpu.SemaphoreType.DMA((4,)),
            pltpu.SemaphoreType.DMA((4,)),
            pltpu.SemaphoreType.DMA((n_dev,)),
            pltpu.SemaphoreType.DMA((n_dev,)),
            pltpu.SemaphoreType.DMA((n_grp,)),
            pltpu.SemaphoreType.DMA((n_grp,)),
        ],
        compiler_params=pltpu.CompilerParams(
            collective_id=0, has_side_effects=True, vmem_limit_bytes=60 * 1024 * 1024
        ),
        name="galerkin",
    )(sidx, wf, elem_slot, tinv, pos, cidx, a_blocks, prolong_t, ms, ma)


def solution(mesh):
    in_specs = (
        P(("grp", "dev"), None, None, None),
        P(("grp", "dev"), None, None),
        P(("grp", "dev")),
        P(),
        P(("grp", "dev"), None),
        P(("grp", "dev"), None),
        P(),
    )
    out_specs = P("dev", None, None)
    return jax.shard_map(
        functools.partial(on_device, mesh.shape["grp"], mesh.shape["dev"]),
        mesh=mesh, in_specs=in_specs, out_specs=out_specs, check_vma=False,
    )
```

```python
import functools

import jax
import jax.numpy as jnp
from jax import lax
from jax.experimental import pallas as pl
from jax.experimental.pallas import tpu as pltpu
from jax.sharding import PartitionSpec as P

EX = 4
EY = 4
MESH = pl.DeviceIdType.MESH
F32 = jnp.float32
BF16 = jnp.bfloat16


def iota(shape, dim):
    return lax.broadcasted_iota(jnp.int32, shape, dim)


def tables(
    n_grp, n_dev, halo, group_rows, rows_own,
    nbr, nbr_agg, slot, touch_agg, coarse_row,
    tab, ms, ma,
):
    grp = lax.axis_index("grp")
    dev = lax.axis_index("dev")
    device = grp * n_dev + dev
    faces, e_dev = nbr.shape
    devices, touch = touch_agg.shape
    wide = ms.shape[1]
    width_c = wide // (faces + 1)

    def where_sum(mask, value, axis):
        return jnp.sum(jnp.where(mask, value, 0), axis=axis, keepdims=True)

    def put(row, value):
        tab[row:row + value.shape[0], 0:value.shape[1]] = value

    near = [
        jnp.where(grp > 0, device - n_dev, -2),
        jnp.where(grp < n_grp - 1, device + n_dev, -2),
        jnp.where(dev > 0, device - 1, -2),
        jnp.where(dev < n_dev - 1, device + 1, -2),
    ]
    ids = nbr[...]
    source = jnp.where(ids >= 0, jnp.maximum(ids, 0) // e_dev, -1)
    local = ids - source * e_dev
    hits = [jnp.max(jnp.where(source == n, 1.0, 0.0), axis=0, keepdims=True) for n in near]
    below = jnp.where(iota((e_dev, e_dev), 0) < iota((e_dev, e_dev), 1), 1.0, 0.0).astype(BF16)
    rank = jnp.dot(
        jnp.concatenate(hits + hits, axis=0).astype(BF16), below, preferred_element_type=F32
    ).astype(jnp.int32)
    lanes = iota((halo, e_dev), 1)
    for d in range(4):
        found = (rank[d:d + 1] == iota((halo, e_dev), 0)) & (hits[d] > 0)
        tab[8:8 + halo, d:d + 1] = where_sum(found, lanes, 1)
    index = iota((e_dev, e_dev), 0)
    where_from = [jnp.where(source[f:f + 1] == device, local[f:f + 1], 0) for f in range(faces)]
    for d in range(4):
        seen = jnp.zeros((e_dev, e_dev), jnp.int32)
        for f in range(faces):
            seen = jnp.where(ids[f:f + 1] == near[d] * e_dev + index, 1, seen)
        seen = jnp.max(seen, axis=1, keepdims=True)
        for f in range(faces):
            ahead = where_sum(index < local[f:f + 1], seen, 0)
            where_from[f] = jnp.where(
                source[f:f + 1] == near[d], e_dev + d * halo + ahead, where_from[f]
            )
    for f in range(faces):
        put(f, where_from[f])

    row = iota((devices, 1), 0)
    entries = touch_agg[...]
    columns = [entries[:, t:t + 1] for t in range(touch)]
    slots = slot[...]
    put(19, slots)
    own_agg = jnp.zeros((1, e_dev), jnp.int32)
    for t in range(touch):
        own_agg = jnp.where(slots == t, where_sum(row == device, columns[t], 0), own_agg)
    valid = ids >= 0
    same = valid & (nbr_agg[...] == own_agg)
    apart = jnp.where(valid & jnp.logical_not(same), 1.0, 0.0).astype(BF16)
    same = jnp.where(same, 1.0, 0.0).astype(BF16)
    unit = jnp.where(iota((e_dev, e_dev), 0) == iota((e_dev, e_dev), 1), 1.0, 0.0).astype(BF16)
    group = jnp.where(iota((faces, wide), 1) // width_c == iota((faces, wide), 0) + 1, 1.0, 0.0).astype(BF16)

    def expand(flags):
        turned = lax.dot_general(unit, flags, (((1,), (1,)), ((), ())), preferred_element_type=F32)
        return jnp.dot(turned.astype(BF16), group, preferred_element_type=F32)

    ms[...] = expand(same) + jnp.where(iota((e_dev, wide), 1) < width_c, 1.0, 0.0)
    ma[...] = expand(apart)

    n_agg = coarse_row.shape[1]
    numbers = coarse_row[...]
    across = iota((devices, n_agg), 1)
    targets = [where_sum(columns[t] == across, numbers, 1) for t in range(touch)]
    owners = [target // rows_own for target in targets]
    lane = iota((devices, rows_own), 1)
    present = jnp.zeros((devices, rows_own), F32)
    for t in range(touch):
        here = jnp.where(owners[t] == dev, targets[t] - owners[t] * rows_own, -1)
        present = jnp.where(here == lane, 1.0, present)
    mates = jnp.where(
        iota((devices, devices), 0) // n_dev == iota((devices, devices), 1) // n_dev, 1.0, 0.0
    ).astype(BF16)
    shared = jnp.dot(mates, present.astype(BF16), preferred_element_type=F32) > 0
    shared = jnp.where(shared, 1.0, 0.0)
    lower = jnp.where(
        iota((rows_own, rows_own), 0) < iota((rows_own, rows_own), 1), 1.0, 0.0
    ).astype(BF16)
    order = jnp.dot(shared.astype(BF16), lower, preferred_element_type=F32)
    heads = where_sum(row % n_dev == 0, shared * (order + 1.0 + (row // n_dev * group_rows).astype(F32)), 0)
    put(16, heads.astype(jnp.int32) - 1)
    spots = jnp.sum(present * (order + 1.0), axis=1, keepdims=True).astype(jnp.int32) - 1
    peer = iota((devices, n_dev), 1) + grp * n_dev
    put(18, where_sum(peer == iota((devices, n_dev), 0), spots, 0))
    inverse = jnp.full((1, n_dev), touch, jnp.int32)
    for t in range(touch):
        own = where_sum(row == device, owners[t], 0)
        inverse = jnp.where(own == iota((1, n_dev), 1), t, inverse)
    put(17, inverse)


def finish(group_rows, tab, gathered, out_ref, flat):
    rows_own, n_k, row_width = out_ref.shape
    lane = 128
    sub = row_width // lane

    @pl.loop(0, rows_own)
    def _(r):
        at = tab[16, r]
        safe = jnp.maximum(at, 0)
        row = gathered[safe // group_rows, safe % group_rows].astype(F32)
        flat[r] = jnp.where(at >= 0, row, 0.0)
        for j in range(sub):
            out_ref[r, :, j * lane:(j + 1) * lane] = flat[r, pl.ds(j, n_k, stride=sub), :]


def kernel(
    n_grp, n_dev, halo, group_rows,
    tab, a_ref, p_ref, ms_ref, ma_ref,
    gathered,
    a_buf, pool, pack, left, prod_s, prod_a, part_t, parts, inbox,
    a_sem, h_send, h_recv, x_send, x_recv, g_send, g_recv,
):
    grp = lax.axis_index("grp")
    dev = lax.axis_index("dev")
    e_dev, width_c, width_b = p_ref.shape
    n_k = a_ref.shape[1]
    touch = part_t.shape[0] - 1
    wide = n_k * width_c
    lane = 128
    rep = lane // width_c
    sub = width_c // rep

    def a_copy(e):
        return pltpu.make_async_copy(a_ref.at[e], a_buf.at[e], a_sem.at[e])

    @pl.loop(0, e_dev)
    def _(e):
        a_copy(e).start()

    barrier = pltpu.get_barrier_semaphore()
    for off in range(1, n_dev):
        pl.semaphore_signal(
            barrier, inc=1, device_id=(grp, lax.rem(dev + off, n_dev)), device_id_type=MESH
        )
    for off in range(1, n_grp):
        pl.semaphore_signal(
            barrier, inc=1, device_id=(lax.rem(grp + off, n_grp), dev), device_id_type=MESH
        )

    for j in range(4 * halo):
        pack[j] = p_ref[tab[8 + j % halo, j // halo]]
    pool[0:e_dev] = p_ref[...]
    pl.semaphore_wait(barrier, n_dev + n_grp - 2)

    dirs = (
        (grp > 0, (grp - 1, dev)),
        (grp < n_grp - 1, (grp + 1, dev)),
        (dev > 0, (grp, dev - 1)),
        (dev < n_dev - 1, (grp, dev + 1)),
    )

    def halo_copy(d, target):
        back = d ^ 1
        return pltpu.make_async_remote_copy(
            src_ref=pack.at[pl.ds(d * halo, halo)],
            dst_ref=pool.at[pl.ds(e_dev + back * halo, halo)],
            send_sem=h_send.at[d],
            recv_sem=h_recv.at[back],
            device_id=target,
            device_id_type=MESH,
        )

    for d, (there, target) in enumerate(dirs):
        @pl.when(there)
        def _(d=d, target=target):
            halo_copy(d, target).start()

    @pl.loop(0, e_dev)
    def _(e):
        a_copy(e).wait()
        own = p_ref[e]
        for k in range(n_k):
            left[e, k * width_c:(k + 1) * width_c, :] = jnp.dot(
                own, a_buf[e, k], preferred_element_type=F32
            ).astype(BF16)

    for d, (there, target) in enumerate(dirs):
        @pl.when(there)
        def _(d=d, target=target):
            halo_copy(d, target).wait_send()
            pltpu.make_async_remote_copy(
                src_ref=pack.at[pl.ds(d * halo, halo)],
                dst_ref=pool.at[pl.ds(e_dev + d * halo, halo)],
                send_sem=h_send.at[d],
                recv_sem=h_recv.at[d],
                device_id=target,
                device_id_type=MESH,
            ).wait_recv()

    group_of_lane = iota((width_c, wide), 1) // width_c

    @pl.loop(0, e_dev)
    def _(e):
        right = jnp.concatenate(
            [pool[e]] + [pool[tab[f, e]] for f in range(n_k - 1)], axis=0
        )
        full = lax.dot_general(
            left[e], right, (((1,), (1,)), ((), ())), preferred_element_type=F32
        )
        picked = full[0:width_c]
        for k in range(1, n_k):
            picked = jnp.where(group_of_lane == k, full[k * width_c:(k + 1) * width_c], picked)
        prod_s[e] = jnp.where(ms_ref[pl.ds(e, 1), :] > 0, picked, 0.0)
        prod_a[e] = jnp.where(ma_ref[pl.ds(e, 1), :] > 0, picked, 0.0)

    spread_s = (iota((wide, lane), 0) % width_c == iota((wide, lane), 1) % width_c).astype(F32).astype(BF16)
    rest = (n_k - 1) * lane
    spread_a = (
        iota((wide, rest), 0)
        == (iota((wide, rest), 1) // lane + 1) * width_c + iota((wide, rest), 1) % width_c
    ).astype(F32).astype(BF16)
    keep = iota((width_c, n_k * lane), 0) % rep == (iota((width_c, n_k * lane), 1) % lane) // width_c
    squeeze = (iota((sub, width_c), 1) // rep == iota((sub, width_c), 0)).astype(F32).astype(BF16)

    part_t[touch] = jnp.zeros(part_t.shape[1:], BF16)

    def spread(value, table):
        high = value.astype(BF16)
        low = (value - high.astype(F32)).astype(BF16)
        return jnp.dot(high, table, preferred_element_type=F32) + jnp.dot(
            low, table, preferred_element_type=F32
        )

    for t in range(touch):
        zero = jnp.zeros((width_c, wide), F32)

        def add(e, sums, t=t):
            sum_s, sum_a = sums
            member = jnp.where(tab[19, e] == t, 1.0, 0.0).astype(F32)
            return sum_s + prod_s[e] * member, sum_a + prod_a[e] * member

        sum_s, sum_a = lax.fori_loop(0, e_dev, add, (zero, zero), unroll=4)
        both = jnp.concatenate([spread(sum_s, spread_s), spread(sum_a, spread_a)], axis=1)
        both = jnp.where(keep, both, 0.0).astype(BF16)
        rows = jnp.dot(squeeze, both, preferred_element_type=F32)
        rows = jnp.concatenate([rows[:, s * lane:(s + 1) * lane] for s in range(n_k)], axis=0)
        part_t[t] = rows.astype(BF16)

    for o in range(n_dev):
        parts[o] = part_t[tab[17, o]]
    inbox[dev] = parts[dev]

    def part_copy(off):
        target = lax.rem(dev + off, n_dev)
        return pltpu.make_async_remote_copy(
            src_ref=parts.at[target],
            dst_ref=inbox.at[dev],
            send_sem=x_send.at[off],
            recv_sem=x_recv.at[off],
            device_id=(grp, target),
            device_id_type=MESH,
        )

    def part_arrival(off):
        sender = lax.rem(dev + n_dev - off, n_dev)
        return pltpu.make_async_remote_copy(
            src_ref=parts.at[sender],
            dst_ref=inbox.at[sender],
            send_sem=x_send.at[off],
            recv_sem=x_recv.at[off],
            device_id=(grp, sender),
            device_id_type=MESH,
        )

    for off in range(1, n_dev):
        part_copy(off).start()
    for off in range(1, n_dev):
        part_arrival(off).wait_recv()

    for j in range(group_rows):
        total = jnp.zeros(parts.shape[1:], F32)
        for d in range(n_dev):
            member = jnp.where(tab[18, d] == j, 1.0, 0.0).astype(F32)
            total = total + inbox[d].astype(F32) * member
        gathered[grp, j] = total.astype(BF16)

    def row_copy(off):
        target = lax.rem(grp + off, n_grp)
        return pltpu.make_async_remote_copy(
            src_ref=gathered.at[grp],
            dst_ref=gathered.at[grp],
            send_sem=g_send.at[off],
            recv_sem=g_recv.at[off],
            device_id=(target, dev),
            device_id_type=MESH,
        )

    def row_arrival(off):
        sender = lax.rem(grp + n_grp - off, n_grp)
        return pltpu.make_async_remote_copy(
            src_ref=gathered.at[sender],
            dst_ref=gathered.at[sender],
            send_sem=g_send.at[off],
            recv_sem=g_recv.at[off],
            device_id=(sender, dev),
            device_id_type=MESH,
        )

    for off in range(1, n_grp):
        row_copy(off).start()
    for off in range(1, n_grp):
        row_arrival(off).wait_recv()

    for off in range(1, n_dev):
        part_copy(off).wait_send()
    for off in range(1, n_grp):
        row_copy(off).wait_send()


def on_device(n_grp, n_dev, a_blocks, prolong_t, elem_slot, touch_agg, nbr, nbr_agg, coarse_row):
    e_dev, width_c, width_b = prolong_t.shape
    n_k = a_blocks.shape[1]
    touch = touch_agg.shape[1]
    halo = e_dev // EX
    half_y = EY // 2
    span_y = half_y + 1
    group_rows = (n_dev * half_y + 1 + half_y) // span_y
    rows_own = n_grp * group_rows
    assert touch <= n_dev
    lane = 128
    flat_rows = n_k * width_c * width_c // lane
    smem = pl.BlockSpec(memory_space=pltpu.SMEM)
    vmem = pl.BlockSpec(memory_space=pltpu.VMEM)
    wide = n_k * width_c
    tab, ms, ma = pl.pallas_call(
        functools.partial(tables, n_grp, n_dev, halo, group_rows, rows_own),
        out_shape=(
            jax.ShapeDtypeStruct((24, lane), jnp.int32),
            jax.ShapeDtypeStruct((e_dev, wide), F32),
            jax.ShapeDtypeStruct((e_dev, wide), F32),
        ),
        in_specs=[vmem] * 5,
        out_specs=(vmem, vmem, vmem),
        name="index_tables",
    )(nbr.T, nbr_agg.T, elem_slot.reshape(1, e_dev), touch_agg, coarse_row.reshape(1, -1))
    gathered = pl.pallas_call(
        functools.partial(kernel, n_grp, n_dev, halo, group_rows),
        out_shape=jax.ShapeDtypeStruct((n_grp, group_rows, flat_rows, lane), BF16),
        in_specs=[smem, pl.BlockSpec(memory_space=pl.ANY)] + [vmem] * 3,
        out_specs=vmem,
        scratch_shapes=[
            pltpu.VMEM(a_blocks.shape, BF16),
            pltpu.VMEM((e_dev + 4 * halo, width_c, width_b), BF16),
            pltpu.VMEM((4 * halo, width_c, width_b), BF16),
            pltpu.VMEM((e_dev, wide, width_b), BF16),
            pltpu.VMEM((e_dev, width_c, wide), F32),
            pltpu.VMEM((e_dev, width_c, wide), F32),
            pltpu.VMEM((touch + 1, flat_rows, lane), BF16),
            pltpu.VMEM((n_dev, flat_rows, lane), BF16),
            pltpu.VMEM((n_dev, flat_rows, lane), BF16),
            pltpu.SemaphoreType.DMA((e_dev,)),
            pltpu.SemaphoreType.DMA((4,)),
            pltpu.SemaphoreType.DMA((4,)),
            pltpu.SemaphoreType.DMA((n_dev,)),
            pltpu.SemaphoreType.DMA((n_dev,)),
            pltpu.SemaphoreType.DMA((n_grp,)),
            pltpu.SemaphoreType.DMA((n_grp,)),
        ],
        compiler_params=pltpu.CompilerParams(
            collective_id=0, has_side_effects=True, vmem_limit_bytes=60 * 1024 * 1024
        ),
        name="galerkin",
    )(tab, a_blocks, prolong_t, ms, ma)
    return pl.pallas_call(
        functools.partial(finish, group_rows),
        out_shape=jax.ShapeDtypeStruct((rows_own, n_k, width_c * width_c), F32),
        in_specs=[smem, vmem],
        out_specs=vmem,
        scratch_shapes=[pltpu.VMEM((rows_own, flat_rows, lane), F32)],
        name="index_finish",
    )(tab, gathered)


def solution(mesh):
    in_specs = (
        P(("grp", "dev"), None, None, None),
        P(("grp", "dev"), None, None),
        P(("grp", "dev")),
        P(),
        P(("grp", "dev"), None),
        P(("grp", "dev"), None),
        P(),
    )
    out_specs = P("dev", None, None)
    return jax.shard_map(
        functools.partial(on_device, mesh.shape["grp"], mesh.shape["dev"]),
        mesh=mesh, in_specs=in_specs, out_specs=out_specs, check_vma=False,
    )
```

```python
import functools

import jax
import jax.numpy as jnp
from jax import lax
from jax.experimental import pallas as pl
from jax.experimental.pallas import tpu as pltpu
from jax.sharding import PartitionSpec as P

EX = 4
EY = 4
MESH = pl.DeviceIdType.MESH
F32 = jnp.float32
BF16 = jnp.bfloat16


def iota(shape, dim):
    return lax.broadcasted_iota(jnp.int32, shape, dim)


def tables(
    n_grp, n_dev, halo, group_rows, rows_own,
    nbr, nbr_agg, slot, touch_agg, coarse_row,
    tab, ms, ma,
):
    grp = lax.axis_index("grp")
    dev = lax.axis_index("dev")
    device = grp * n_dev + dev
    faces, e_dev = nbr.shape
    devices, touch = touch_agg.shape
    wide = ms.shape[1]
    width_c = wide // (faces + 1)

    def where_sum(mask, value, axis):
        return jnp.sum(jnp.where(mask, value, 0), axis=axis, keepdims=True)

    def put(row, value):
        tab[row:row + value.shape[0], 0:value.shape[1]] = value

    near = [
        jnp.where(grp > 0, device - n_dev, -2),
        jnp.where(grp < n_grp - 1, device + n_dev, -2),
        jnp.where(dev > 0, device - 1, -2),
        jnp.where(dev < n_dev - 1, device + 1, -2),
    ]
    ids = nbr[...]
    source = jnp.where(ids >= 0, jnp.maximum(ids, 0) // e_dev, -1)
    local = ids - source * e_dev
    hits = [jnp.max(jnp.where(source == n, 1.0, 0.0), axis=0, keepdims=True) for n in near]
    below = jnp.where(iota((e_dev, e_dev), 0) < iota((e_dev, e_dev), 1), 1.0, 0.0).astype(BF16)
    rank = jnp.dot(
        jnp.concatenate(hits + hits, axis=0).astype(BF16), below, preferred_element_type=F32
    ).astype(jnp.int32)
    lanes = iota((halo, e_dev), 1)
    for d in range(4):
        found = (rank[d:d + 1] == iota((halo, e_dev), 0)) & (hits[d] > 0)
        tab[8:8 + halo, d:d + 1] = where_sum(found, lanes, 1)
    index = iota((e_dev, e_dev), 0)
    where_from = [jnp.where(source[f:f + 1] == device, local[f:f + 1], 0) for f in range(faces)]
    for d in range(4):
        seen = jnp.zeros((e_dev, e_dev), jnp.int32)
        for f in range(faces):
            seen = jnp.where(ids[f:f + 1] == near[d] * e_dev + index, 1, seen)
        seen = jnp.max(seen, axis=1, keepdims=True)
        for f in range(faces):
            ahead = where_sum(index < local[f:f + 1], seen, 0)
            where_from[f] = jnp.where(
                source[f:f + 1] == near[d], e_dev + d * halo + ahead, where_from[f]
            )
    for f in range(faces):
        put(f, where_from[f])

    row = iota((devices, 1), 0)
    entries = touch_agg[...]
    columns = [entries[:, t:t + 1] for t in range(touch)]
    slots = slot[...]
    put(19, slots)
    own_agg = jnp.zeros((1, e_dev), jnp.int32)
    for t in range(touch):
        own_agg = jnp.where(slots == t, where_sum(row == device, columns[t], 0), own_agg)
    valid = ids >= 0
    same = valid & (nbr_agg[...] == own_agg)
    apart = jnp.where(valid & jnp.logical_not(same), 1.0, 0.0).astype(BF16)
    same = jnp.where(same, 1.0, 0.0).astype(BF16)
    unit = jnp.where(iota((e_dev, e_dev), 0) == iota((e_dev, e_dev), 1), 1.0, 0.0).astype(BF16)
    group = jnp.where(iota((faces, wide), 1) // width_c == iota((faces, wide), 0) + 1, 1.0, 0.0).astype(BF16)

    def expand(flags):
        turned = lax.dot_general(unit, flags, (((1,), (1,)), ((), ())), preferred_element_type=F32)
        return jnp.dot(turned.astype(BF16), group, preferred_element_type=F32)

    ms[...] = expand(same) + jnp.where(iota((e_dev, wide), 1) < width_c, 1.0, 0.0)
    ma[...] = expand(apart)

    n_agg = coarse_row.shape[1]
    numbers = coarse_row[...]
    across = iota((devices, n_agg), 1)
    targets = [where_sum(columns[t] == across, numbers, 1) for t in range(touch)]
    owners = [target // rows_own for target in targets]
    lane = iota((devices, rows_own), 1)
    present = jnp.zeros((devices, rows_own), F32)
    for t in range(touch):
        here = jnp.where(owners[t] == dev, targets[t] - owners[t] * rows_own, -1)
        present = jnp.where(here == lane, 1.0, present)
    mates = jnp.where(
        iota((devices, devices), 0) // n_dev == iota((devices, devices), 1) // n_dev, 1.0, 0.0
    ).astype(BF16)
    shared = jnp.dot(mates, present.astype(BF16), preferred_element_type=F32) > 0
    shared = jnp.where(shared, 1.0, 0.0)
    lower = jnp.where(
        iota((rows_own, rows_own), 0) < iota((rows_own, rows_own), 1), 1.0, 0.0
    ).astype(BF16)
    order = jnp.dot(shared.astype(BF16), lower, preferred_element_type=F32)
    heads = where_sum(row % n_dev == 0, shared * (order + 1.0 + (row // n_dev * group_rows).astype(F32)), 0)
    put(16, heads.astype(jnp.int32) - 1)
    spots = jnp.sum(present * (order + 1.0), axis=1, keepdims=True).astype(jnp.int32) - 1
    peer = iota((devices, n_dev), 1) + grp * n_dev
    put(18, where_sum(peer == iota((devices, n_dev), 0), spots, 0))
    inverse = jnp.full((1, n_dev), touch, jnp.int32)
    for t in range(touch):
        own = where_sum(row == device, owners[t], 0)
        inverse = jnp.where(own == iota((1, n_dev), 1), t, inverse)
    put(17, inverse)


def finish(group_rows, tab, gathered, out_ref, flat):
    rows_own, n_k, row_width = out_ref.shape
    lane = 128
    sub = row_width // lane

    @pl.loop(0, rows_own, unroll=4)
    def _(r):
        at = tab[16, r]
        safe = jnp.maximum(at, 0)
        row = gathered[safe // group_rows, safe % group_rows].astype(F32)
        flat[r] = jnp.where(at >= 0, row, 0.0)
        for j in range(sub):
            out_ref[r, :, j * lane:(j + 1) * lane] = flat[r, pl.ds(j, n_k, stride=sub), :]


def kernel(
    n_grp, n_dev, halo, group_rows,
    tab, a_ref, p_ref, ms_ref, ma_ref,
    gathered,
    a_buf, pool, pack, left, prod_s, prod_a, part_t, parts, inbox,
    a_sem, h_send, h_recv, x_send, x_recv, g_send, g_recv,
):
    grp = lax.axis_index("grp")
    dev = lax.axis_index("dev")
    e_dev, width_c, width_b = p_ref.shape
    n_k = a_ref.shape[1]
    touch = part_t.shape[0] - 1
    wide = n_k * width_c
    lane = 128
    rep = lane // width_c
    sub = width_c // rep

    def a_copy(e):
        return pltpu.make_async_copy(a_ref.at[e], a_buf.at[e], a_sem.at[e])

    @pl.loop(0, e_dev)
    def _(e):
        a_copy(e).start()

    barrier = pltpu.get_barrier_semaphore()
    for off in range(1, n_dev):
        pl.semaphore_signal(
            barrier, inc=1, device_id=(grp, lax.rem(dev + off, n_dev)), device_id_type=MESH
        )
    for off in range(1, n_grp):
        pl.semaphore_signal(
            barrier, inc=1, device_id=(lax.rem(grp + off, n_grp), dev), device_id_type=MESH
        )

    for j in range(4 * halo):
        pack[j] = p_ref[tab[8 + j % halo, j // halo]]
    pool[0:e_dev] = p_ref[...]
    pl.semaphore_wait(barrier, n_dev + n_grp - 2)

    dirs = (
        (grp > 0, (grp - 1, dev)),
        (grp < n_grp - 1, (grp + 1, dev)),
        (dev > 0, (grp, dev - 1)),
        (dev < n_dev - 1, (grp, dev + 1)),
    )

    def halo_copy(d, target):
        back = d ^ 1
        return pltpu.make_async_remote_copy(
            src_ref=pack.at[pl.ds(d * halo, halo)],
            dst_ref=pool.at[pl.ds(e_dev + back * halo, halo)],
            send_sem=h_send.at[d],
            recv_sem=h_recv.at[back],
            device_id=target,
            device_id_type=MESH,
        )

    for d, (there, target) in enumerate(dirs):
        @pl.when(there)
        def _(d=d, target=target):
            halo_copy(d, target).start()

    @pl.loop(0, e_dev, unroll=2)
    def _(e):
        a_copy(e).wait()
        own = p_ref[e]
        for k in range(n_k):
            left[e, k * width_c:(k + 1) * width_c, :] = jnp.dot(
                own, a_buf[e, k], preferred_element_type=F32
            ).astype(BF16)

    for d, (there, target) in enumerate(dirs):
        @pl.when(there)
        def _(d=d, target=target):
            halo_copy(d, target).wait_send()
            pltpu.make_async_remote_copy(
                src_ref=pack.at[pl.ds(d * halo, halo)],
                dst_ref=pool.at[pl.ds(e_dev + d * halo, halo)],
                send_sem=h_send.at[d],
                recv_sem=h_recv.at[d],
                device_id=target,
                device_id_type=MESH,
            ).wait_recv()

    group_of_lane = iota((width_c, wide), 1) // width_c

    @pl.loop(0, e_dev, unroll=4)
    def _(e):
        right = jnp.concatenate(
            [pool[e]] + [pool[tab[f, e]] for f in range(n_k - 1)], axis=0
        )
        full = lax.dot_general(
            left[e], right, (((1,), (1,)), ((), ())), preferred_element_type=F32
        )
        picked = full[0:width_c]
        for k in range(1, n_k):
            picked = jnp.where(group_of_lane == k, full[k * width_c:(k + 1) * width_c], picked)
        prod_s[e] = jnp.where(ms_ref[pl.ds(e, 1), :] > 0, picked, 0.0)
        prod_a[e] = jnp.where(ma_ref[pl.ds(e, 1), :] > 0, picked, 0.0)

    spread_s = (iota((wide, lane), 0) % width_c == iota((wide, lane), 1) % width_c).astype(F32).astype(BF16)
    rest = (n_k - 1) * lane
    spread_a = (
        iota((wide, rest), 0)
        == (iota((wide, rest), 1) // lane + 1) * width_c + iota((wide, rest), 1) % width_c
    ).astype(F32).astype(BF16)
    keep = iota((width_c, n_k * lane), 0) % rep == (iota((width_c, n_k * lane), 1) % lane) // width_c
    squeeze = (iota((sub, width_c), 1) // rep == iota((sub, width_c), 0)).astype(F32).astype(BF16)

    part_t[touch] = jnp.zeros(part_t.shape[1:], BF16)

    def spread(value, table):
        high = value.astype(BF16)
        low = (value - high.astype(F32)).astype(BF16)
        return jnp.dot(high, table, preferred_element_type=F32) + jnp.dot(
            low, table, preferred_element_type=F32
        )

    for t in range(touch):
        zero = jnp.zeros((width_c, wide), F32)

        def add(e, sums, t=t):
            sum_s, sum_a = sums
            member = jnp.where(tab[19, e] == t, 1.0, 0.0).astype(F32)
            return sum_s + prod_s[e] * member, sum_a + prod_a[e] * member

        sum_s, sum_a = lax.fori_loop(0, e_dev, add, (zero, zero), unroll=8)
        both = jnp.concatenate([spread(sum_s, spread_s), spread(sum_a, spread_a)], axis=1)
        both = jnp.where(keep, both, 0.0).astype(BF16)
        rows = jnp.dot(squeeze, both, preferred_element_type=F32)
        rows = jnp.concatenate([rows[:, s * lane:(s + 1) * lane] for s in range(n_k)], axis=0)
        part_t[t] = rows.astype(BF16)

    for o in range(n_dev):
        parts[o] = part_t[tab[17, o]]
    inbox[dev] = parts[dev]

    def part_copy(off):
        target = lax.rem(dev + off, n_dev)
        return pltpu.make_async_remote_copy(
            src_ref=parts.at[target],
            dst_ref=inbox.at[dev],
            send_sem=x_send.at[off],
            recv_sem=x_recv.at[off],
            device_id=(grp, target),
            device_id_type=MESH,
        )

    def part_arrival(off):
        sender = lax.rem(dev + n_dev - off, n_dev)
        return pltpu.make_async_remote_copy(
            src_ref=parts.at[sender],
            dst_ref=inbox.at[sender],
            send_sem=x_send.at[off],
            recv_sem=x_recv.at[off],
            device_id=(grp, sender),
            device_id_type=MESH,
        )

    for off in range(1, n_dev):
        part_copy(off).start()
    for off in range(1, n_dev):
        part_arrival(off).wait_recv()

    for j in range(group_rows):
        total = jnp.zeros(parts.shape[1:], F32)
        for d in range(n_dev):
            member = jnp.where(tab[18, d] == j, 1.0, 0.0).astype(F32)
            total = total + inbox[d].astype(F32) * member
        gathered[grp, j] = total.astype(BF16)

    def row_copy(off):
        target = lax.rem(grp + off, n_grp)
        return pltpu.make_async_remote_copy(
            src_ref=gathered.at[grp],
            dst_ref=gathered.at[grp],
            send_sem=g_send.at[off],
            recv_sem=g_recv.at[off],
            device_id=(target, dev),
            device_id_type=MESH,
        )

    def row_arrival(off):
        sender = lax.rem(grp + n_grp - off, n_grp)
        return pltpu.make_async_remote_copy(
            src_ref=gathered.at[sender],
            dst_ref=gathered.at[sender],
            send_sem=g_send.at[off],
            recv_sem=g_recv.at[off],
            device_id=(sender, dev),
            device_id_type=MESH,
        )

    for off in range(1, n_grp):
        row_copy(off).start()
    for off in range(1, n_grp):
        row_arrival(off).wait_recv()

    for off in range(1, n_dev):
        part_copy(off).wait_send()
    for off in range(1, n_grp):
        row_copy(off).wait_send()


def on_device(n_grp, n_dev, a_blocks, prolong_t, elem_slot, touch_agg, nbr, nbr_agg, coarse_row):
    e_dev, width_c, width_b = prolong_t.shape
    n_k = a_blocks.shape[1]
    touch = touch_agg.shape[1]
    halo = e_dev // EX
    half_y = EY // 2
    span_y = half_y + 1
    group_rows = (n_dev * half_y + 1 + half_y) // span_y
    rows_own = n_grp * group_rows
    assert touch <= n_dev
    lane = 128
    flat_rows = n_k * width_c * width_c // lane
    smem = pl.BlockSpec(memory_space=pltpu.SMEM)
    vmem = pl.BlockSpec(memory_space=pltpu.VMEM)
    wide = n_k * width_c
    tab, ms, ma = pl.pallas_call(
        functools.partial(tables, n_grp, n_dev, halo, group_rows, rows_own),
        out_shape=(
            jax.ShapeDtypeStruct((24, lane), jnp.int32),
            jax.ShapeDtypeStruct((e_dev, wide), F32),
            jax.ShapeDtypeStruct((e_dev, wide), F32),
        ),
        in_specs=[vmem] * 5,
        out_specs=(vmem, vmem, vmem),
        name="index_tables",
    )(nbr.T, nbr_agg.T, elem_slot.reshape(1, e_dev), touch_agg, coarse_row.reshape(1, -1))
    gathered = pl.pallas_call(
        functools.partial(kernel, n_grp, n_dev, halo, group_rows),
        out_shape=jax.ShapeDtypeStruct((n_grp, group_rows, flat_rows, lane), BF16),
        in_specs=[smem, pl.BlockSpec(memory_space=pl.ANY)] + [vmem] * 3,
        out_specs=vmem,
        scratch_shapes=[
            pltpu.VMEM(a_blocks.shape, BF16),
            pltpu.VMEM((e_dev + 4 * halo, width_c, width_b), BF16),
            pltpu.VMEM((4 * halo, width_c, width_b), BF16),
            pltpu.VMEM((e_dev, wide, width_b), BF16),
            pltpu.VMEM((e_dev, width_c, wide), F32),
            pltpu.VMEM((e_dev, width_c, wide), F32),
            pltpu.VMEM((touch + 1, flat_rows, lane), BF16),
            pltpu.VMEM((n_dev, flat_rows, lane), BF16),
            pltpu.VMEM((n_dev, flat_rows, lane), BF16),
            pltpu.SemaphoreType.DMA((e_dev,)),
            pltpu.SemaphoreType.DMA((4,)),
            pltpu.SemaphoreType.DMA((4,)),
            pltpu.SemaphoreType.DMA((n_dev,)),
            pltpu.SemaphoreType.DMA((n_dev,)),
            pltpu.SemaphoreType.DMA((n_grp,)),
            pltpu.SemaphoreType.DMA((n_grp,)),
        ],
        compiler_params=pltpu.CompilerParams(
            collective_id=0, has_side_effects=True, vmem_limit_bytes=60 * 1024 * 1024
        ),
        name="galerkin",
    )(tab, a_blocks, prolong_t, ms, ma)
    return pl.pallas_call(
        functools.partial(finish, group_rows),
        out_shape=jax.ShapeDtypeStruct((rows_own, n_k, width_c * width_c), F32),
        in_specs=[smem, vmem],
        out_specs=vmem,
        scratch_shapes=[pltpu.VMEM((rows_own, flat_rows, lane), F32)],
        name="index_finish",
    )(tab, gathered)


def solution(mesh):
    in_specs = (
        P(("grp", "dev"), None, None, None),
        P(("grp", "dev"), None, None),
        P(("grp", "dev")),
        P(),
        P(("grp", "dev"), None),
        P(("grp", "dev"), None),
        P(),
    )
    out_specs = P("dev", None, None)
    return jax.shard_map(
        functools.partial(on_device, mesh.shape["grp"], mesh.shape["dev"]),
        mesh=mesh, in_specs=in_specs, out_specs=out_specs, check_vma=False,
    )
```
